32 devices in a mesh: lat: 4 (over y, x), ord: 4 (over z), batch: 2 (over core).
Axes of the slice: x: 2, y: 2, z: 4, core: 2. Of those that a mesh axis runs over, the one named last changes fastest.
Arguments:
- state_field: bfloat16 [512, 720, 1440], P(('batch', 'ord'), 'lat'), parts along dimension 0, may hold values from -6 to 6
- slot_order: int32 [512], replicated, may hold values from 0 to 511, each once
- legendre: bfloat16 [512, 720, 720], P(('lat', 'ord')), may hold values from -0.21875 to 0.21875
- degree_gain: float32 [720, 256], replicated, may hold values from 0.25 to 1.75
- mixing: bfloat16 [256, 256], replicated, may hold values from -0.375 to 0.375
Outputs:
- updated: bfloat16 [512, 720, 1440], P(('batch', 'ord'), 'lat'), parts along dimension 0
The draws below stay inside these ranges and needn't reach their ends.
There are 2 independent parts, one for each index of `batch`. The reference program is written for one: setup_inputs(seed, part) draws one part's arguments, and reference() takes and returns one part's arrays. A program takes and returns all parts, laid end to end along the dimension named above; an argument that names none is the same for every part. Nothing has to cross between parts.
Inputs may be any that keep to these rules, and one draw needn't show every extreme that they name: `slot_order`: each of 0 to 511 stands once.
All inputs are finite; a program needn't handle non-finite values.
Results may differ from the reference program's by a relative error of at most 0.0054.
Values may be sent and summed in bfloat16 or wider, within the bound.
A program may use at most 320 MiB of HBM per device.

```python
import math
import jax
import jax.numpy as jnp
from jax import lax

C = 256
NLAT = 720
NLON = 1440
L = 720
M = 512


def level_of(own_key, shape, pieces, low, high):
    def one(axis_at, shards_of):
        steps = jax.random.uniform(jax.random.fold_in(jax.random.fold_in(own_key, 6), axis_at), (shards_of,), jnp.float32, low / len(pieces), high / len(pieces))
        return jnp.repeat(jnp.exp(steps), shape[axis_at] // shards_of).reshape((-1,) + (1,) * (len(shape) - axis_at - 1))

    level = one(*pieces[0])
    for cut in pieces[1:]:
        level = level * one(*cut)
    return level


def normal_values(key, extent, scale, bound, split=(), kind=jnp.bfloat16):
    gain = level_of(key, extent, split, -0.22, 0.18) if split else 1.0
    drawn = jax.random.normal(key, extent, jnp.float32) * scale * gain
    return jnp.minimum(jnp.maximum(drawn, -bound), bound).astype(kind)


def setup_inputs(seed: int = 0, part: int = 0) -> dict:
    seeds = jax.random.split(jax.random.key(seed), 6)
    part_splits = jax.random.split(jax.random.fold_in(seeds[5], part), 6)
    return {
        "state_field": normal_values(part_splits[0], (C, NLAT, NLON), 1.0, 6.0, ((0, 4), (1, 4))),
        "slot_order": jax.random.permutation(seeds[1], M).astype(jnp.int32),
        "legendre": normal_values(seeds[2], (M, L, NLAT), NLAT ** -0.5, 0.21875, ((0, 16),)),
        "degree_gain": jnp.clip(jax.random.uniform(seeds[3], (L, C), jnp.float32, 0.25, 1.75), 0.25, 1.75),
        "mixing": normal_values(seeds[4], (C, C), C ** -0.5, 0.375),
    }


def tables(orders, lon_count):
    longitude = jnp.arange(lon_count, dtype=jnp.int32)
    phase = longitude[:, None] * orders[None, :].astype(jnp.int32) % lon_count
    angle = phase.astype(jnp.float32) * (2.0 * math.pi / lon_count)
    root = 1.0 / math.sqrt(lon_count)
    forward = jnp.concatenate([jnp.cos(angle) * root, -jnp.sin(angle) * root], axis=1).astype(jnp.bfloat16)
    weights = jnp.where(orders == 0, 1.0, 2.0).astype(jnp.float32) * root
    inverse = jnp.concatenate([jnp.cos(angle).T * weights[:, None], -jnp.sin(angle).T * weights[:, None]], axis=0).astype(jnp.bfloat16)
    return (forward, inverse)

def reference(state_field, slot_order, legendre, degree_gain, mixing):
    high = lax.Precision.HIGHEST
    forward, inverse = tables(slot_order, NLON)
    flat = state_field.reshape(C * NLAT, NLON).astype(jnp.float32)
    fourier = jnp.dot(flat, forward.astype(jnp.float32), precision=high, preferred_element_type=jnp.float32).astype(jnp.bfloat16)
    fourier = fourier.reshape(C, NLAT, 2, M).transpose(3, 1, 2, 0).reshape(M, NLAT, 2 * C)
    padded_gain = jnp.concatenate([degree_gain, jnp.zeros((L, C), jnp.float32)], axis=0)
    mix_wide = mixing.astype(jnp.float32)

    def per_slot(item):
        slot_table, coeffs, order = item
        table_wide = slot_table.astype(jnp.float32)
        spec = jnp.dot(table_wide, coeffs.astype(jnp.float32), precision=high, preferred_element_type=jnp.float32)
        gain_rows = lax.dynamic_slice_in_dim(padded_gain, order.astype(jnp.int32), L, 0)
        kept = jnp.arange(L, dtype=jnp.int32) < (L - order).astype(jnp.int32)
        filtered = jnp.where(kept[:, None, None], spec.reshape(L, 2, C) * gain_rows[:, None, :], jnp.float32(0.0)).astype(jnp.bfloat16)
        mixed = jnp.dot(filtered.reshape(2 * L, C).astype(jnp.float32), mix_wide, precision=high, preferred_element_type=jnp.float32)
        mixed = mixed.astype(jnp.bfloat16).reshape(L, 2 * C)
        synth = jnp.dot(table_wide.T, mixed.astype(jnp.float32), precision=high, preferred_element_type=jnp.float32)
        return synth.astype(jnp.bfloat16)
    synth = lax.map(per_slot, (legendre, fourier, slot_order))
    synth = synth.reshape(M, NLAT, 2, C).transpose(3, 1, 2, 0).reshape(C * NLAT, 2 * M)
    back = jnp.dot(synth.astype(jnp.float32), inverse.astype(jnp.float32), precision=high, preferred_element_type=jnp.float32)
    back = back.reshape(C, NLAT, NLON)
    return (state_field.astype(jnp.float32) + jax.nn.gelu(back, approximate=True)).astype(jnp.bfloat16)
```

```python
import functools
import math

import jax
import jax.numpy as jnp
from jax import lax
from jax.experimental import pallas as pl
from jax.experimental.pallas import tpu as pltpu
from jax.sharding import PartitionSpec as P

CHUNKS = 4


def table(orders, lon_count):
    longitude = lax.broadcasted_iota(jnp.int32, orders.shape + (lon_count,), orders.ndim)
    product = (orders[..., None] * longitude).astype(jnp.float32)
    turns = jnp.floor((product + 0.5) * (1.0 / lon_count))
    angle = (product - turns * lon_count) * (2.0 * math.pi / lon_count)
    root = 1.0 / math.sqrt(lon_count)
    return (jnp.cos(angle) * root).astype(jnp.bfloat16), (-jnp.sin(angle) * root).astype(jnp.bfloat16)


def middle_kernel(orders_ref, coeffs_ref, legendre_ref, gain_ref, mixing_ref, out_ref):
    order = orders_ref[pl.program_id(0)]
    slot_table = legendre_ref[0]
    mixing = mixing_ref[...]
    degrees = slot_table.shape[0]
    width = mixing.shape[0]
    weight = jnp.where(order == 0, 1.0, 2.0).astype(jnp.float32)
    kept = lax.broadcasted_iota(jnp.int32, (degrees, width), 0) < degrees - order
    start = pl.multiple_of(order // 8 * 8, 8)
    window = gain_ref[pl.ds(start, degrees + 8), :]
    gain = pltpu.roll(window, degrees + 8 - order % 8, 0)[:degrees]
    for part in range(2):
        spec = lax.dot_general(
            slot_table, coeffs_ref[0, part], (((1,), (0,)), ((), ())), preferred_element_type=jnp.float32
        )
        filtered = jnp.where(kept, spec * gain, 0.0).astype(jnp.bfloat16)
        mixed = jnp.dot(filtered, mixing, preferred_element_type=jnp.float32).astype(jnp.bfloat16)
        synth = lax.dot_general(
            slot_table, mixed, (((0,), (0,)), ((), ())), preferred_element_type=jnp.float32
        )
        out_ref[0, part] = (synth * weight).astype(jnp.bfloat16)


def middle(orders, coeffs, legendre, first, padded_gain, mixing):
    slots, parts, latitudes, width = coeffs.shape
    degrees = legendre.shape[1]
    return pl.pallas_call(
        middle_kernel,
        out_shape=jax.ShapeDtypeStruct(coeffs.shape, jnp.bfloat16),
        grid_spec=pltpu.PrefetchScalarGridSpec(
            num_scalar_prefetch=1,
            grid=(slots,),
            in_specs=[
                pl.BlockSpec((1, parts, latitudes, width), lambda s, o: (s, 0, 0, 0)),
                pl.BlockSpec((1, degrees, latitudes), lambda s, o: (first + s, 0, 0)),
                pl.BlockSpec(padded_gain.shape, lambda s, o: (0, 0)),
                pl.BlockSpec(mixing.shape, lambda s, o: (0, 0)),
            ],
            out_specs=pl.BlockSpec((1, parts, latitudes, width), lambda s, o: (s, 0, 0, 0)),
        ),
        compiler_params=pltpu.CompilerParams(vmem_limit_bytes=40 * 1024 * 1024),
        cost_estimate=pl.CostEstimate(
            flops=2 * slots * parts * width * degrees * (2 * latitudes + width),
            bytes_accessed=2 * slots * latitudes * (2 * parts * width + degrees),
            transcendentals=0,
        ),
    )(orders, coeffs, legendre, padded_gain, mixing)


def plain_shards(state_field, slot_order, legendre, degree_gain, mixing):
    channels, lat_rows, lon_count = state_field.shape
    all_slots = slot_order.shape[0]
    my_slots, degrees, latitudes = legendre.shape
    width = mixing.shape[0]
    lat_count = lax.axis_size("lat")
    ord_count = lax.axis_size("ord")
    devices = lat_count * ord_count
    chunks = math.gcd(CHUNKS, my_slots)
    piece = my_slots // chunks
    rows = channels * lat_rows
    me = lax.axis_index(("lat", "ord"))
    grid_rows = state_field.transpose(1, 0, 2).reshape(rows, lon_count)
    orders_by_device = slot_order.reshape(devices, chunks, piece)
    padded_gain = jnp.concatenate([degree_gain, jnp.zeros((degrees + 8, width), jnp.float32)], axis=0)

    tables = []
    arrived = []
    for g in range(chunks):
        cosine, sine = table(orders_by_device[:, g], lon_count)
        rows_here = jnp.stack([cosine, sine], axis=1).reshape(2 * devices * piece, lon_count)
        tables.append(rows_here)
        fourier = lax.dot_general(
            rows_here, grid_rows, (((1,), (1,)), ((), ())), preferred_element_type=jnp.float32
        ).astype(jnp.bfloat16)
        arrived.append(
            lax.all_to_all(
                fourier.reshape(devices, 2 * piece, rows),
                ("lat", "ord"),
                split_axis=0,
                concat_axis=0,
                tiled=True,
            )
        )

    returned = []
    for g in range(chunks):
        coeffs = arrived[g].reshape(lat_count, ord_count, 2, piece, lat_rows, channels)
        coeffs = coeffs.transpose(3, 2, 0, 4, 1, 5).reshape(piece, 2, latitudes, width)
        orders_here = lax.dynamic_slice_in_dim(slot_order, me * my_slots + g * piece, piece, 0)
        synth = middle(orders_here, coeffs, legendre, g * piece, padded_gain, mixing)
        outgoing = synth.reshape(piece, 2, lat_count, lat_rows, ord_count, channels)
        outgoing = outgoing.transpose(2, 4, 1, 0, 3, 5).reshape(devices, 2 * piece, rows)
        returned.append(
            lax.all_to_all(outgoing, ("lat", "ord"), split_axis=0, concat_axis=0, tiled=True).reshape(
                2 * devices * piece, rows
            )
        )

    back = lax.dot_general(
        jnp.concatenate(returned, axis=0),
        jnp.concatenate(tables, axis=0),
        (((0,), (0,)), ((), ())),
        preferred_element_type=jnp.float32,
    )
    back = back.reshape(lat_rows, channels, lon_count).transpose(1, 0, 2)
    return (state_field.astype(jnp.float32) + jax.nn.gelu(back, approximate=True)).astype(
        jnp.bfloat16
    )


MESH = pl.DeviceIdType.MESH
GROUP = 8
TILE = 15
BLOCK = 5


def order_of_sends(lat_count, ord_count):
    steps = sorted(range(ord_count), key=lambda dz: (dz == 0, abs(2 * dz - ord_count)))
    return [(dl, dz) for dz in steps for dl in range(lat_count) if (dl, dz) != (0, 0)]


def cuts_of(tiles):
    counts = [2] * ((tiles - 2) // 2) + [1] * (tiles % 2 + 2)
    return [(sum(counts[:k]), count) for k, count in enumerate(counts)]


def cosine(phase, lon_count):
    turns = jnp.floor((phase + 0.5) * (1.0 / lon_count))
    fold = jnp.abs(phase - turns * lon_count - lon_count // 2) - lon_count // 4
    angle = fold * (2.0 * math.pi / lon_count)
    square = angle * angle
    series = 1.0 / math.factorial(13)
    for n in (11, 9, 7, 5, 3, 1):
        series = series * square + (-1.0) ** (n // 2) / math.factorial(n)
    return series * angle


def whole_kernel(
    sizes, x_ref, rows_ref, legendre_ref, degree_gain_ref, mixing_ref,
    out_ref, fs_ref, cb_ref, ys_ref, yb_ref,
    table_ref, gains, xv, stage, av, z, legv, rhs, v,
    gain_sem, x_sem, stage_sem, a_sem, leg_sem, v_sem, o_sem, own_sem,
    send_f, recv_f, send_r, recv_r, recv_last,
):
    lat_count, ord_count, groups, half, channels, slots = sizes
    devices = lat_count * ord_count
    lanes = 2 * channels
    pair_rows = 2 * GROUP
    width = ord_count * channels
    degrees = legendre_ref.shape[1]
    order_bits = (devices * slots - 1).bit_length()
    lon_count = x_ref.shape[2]
    tiles = half // TILE
    la = lax.axis_index("lat")
    oz = lax.axis_index("ord")
    bt = lax.axis_index("batch")
    first_slot = (la * ord_count + oz) * slots
    sends = order_of_sends(lat_count, ord_count)
    cuts = cuts_of(tiles)

    def ahead(dl, dz):
        return ((la + dl) % lat_count, (oz + dz) % ord_count, bt)

    def behind(dl, dz):
        return ((la + (lat_count - dl)) % lat_count, (oz + (ord_count - dz)) % ord_count, bt)

    def x_copies(tile, slot):
        return [
            pltpu.make_async_copy(
                x_ref.at[pl.ds(h * half + tile * TILE, TILE)], xv.at[slot, :, h], x_sem.at[slot, h]
            )
            for h in range(2)
        ]

    def leg_copy(q, slot):
        return pltpu.make_async_copy(legendre_ref.at[q], legv.at[slot], leg_sem.at[slot])

    for c in x_copies(0, 0):
        c.start()
    leg_copy(0, 0).start()
    gain_copy = pltpu.make_async_copy(degree_gain_ref, gains.at[pl.ds(0, degrees)], gain_sem)
    gain_copy.start()
    gains[degrees:, :] = jnp.zeros((gains.shape[0] - degrees, width), jnp.float32)

    barrier = pltpu.get_barrier_semaphore()
    for dl, dz in sends:
        pl.semaphore_signal(barrier, inc=1, device_id=ahead(dl, dz), device_id_type=MESH)
    pl.semaphore_wait(barrier, devices - 1)

    def send(src, dst, part, dest, ssem, rsem):
        pltpu.make_async_remote_copy(
            src_ref=src.at[part], dst_ref=dst.at[part], send_sem=ssem, recv_sem=rsem,
            device_id=dest, device_id_type=MESH,
        ).start()

    def send_forward(g):
        for dl, dz in sends:
            part = (g, dl * ord_count + dz)
            send(fs_ref, cb_ref, part, ahead(dl, dz), send_f.at[g], recv_f.at[g])

    def send_back(g):
        for dl, dz in sends:
            part = (g, dl * ord_count + dz)
            send(ys_ref, yb_ref, part, behind(dl, dz), send_r.at[g], recv_r.at[g])

    def table_block(g, k):
        here = pl.ds(pl.multiple_of((g * devices + k) * pair_rows, pair_rows), pair_rows)
        dl, dz = k // ord_count, k % ord_count
        owner = (la + dl) % lat_count * ord_count + (oz + dz) % ord_count
        theirs = (owner * slots + g * GROUP) * 2
        order = rows_ref[pl.ds(pl.multiple_of(theirs, pair_rows), pair_rows), :1]
        shape = (pair_rows, lon_count)
        part = (lax.broadcasted_iota(jnp.int32, shape, 0) % 2).astype(jnp.float32)
        longitude = lax.broadcasted_iota(jnp.int32, shape, 1).astype(jnp.float32)
        values = cosine(order * longitude + part * (lon_count // 4), lon_count)
        table_ref[here, :] = (values * (1.0 / math.sqrt(lon_count))).astype(jnp.bfloat16)

    def forward_step(t, carry):
        g = t // tiles

        @pl.when(t % tiles == 0)
        def _():
            def per_device(k, carry):
                table_block(g, k)
                return carry

            lax.fori_loop(0, devices, per_device, 0)

        table_rows = pl.ds(pl.multiple_of(g * devices * pair_rows, devices * pair_rows), devices * pair_rows)
        tile = t % tiles
        slot = t % 2

        @pl.when(t + 1 < groups * tiles)
        def _():
            for c in x_copies((t + 1) % tiles, (t + 1) % 2):
                c.start()

        for c in x_copies(tile, slot):
            c.wait()

        def block(kb, carry):
            rows = xv[slot, pl.ds(kb * BLOCK, BLOCK)].reshape(BLOCK * lanes, lon_count)
            res = lax.dot_general(
                table_ref[table_rows, :], rows, (((1,), (1,)), ((), ())), preferred_element_type=jnp.float32
            )
            for k in range(BLOCK):
                piece = res[:, k * lanes : (k + 1) * lanes].reshape(devices, pair_rows, lanes)
                stage[:, kb * BLOCK + k] = piece.astype(jnp.bfloat16)
            return carry

        lax.fori_loop(0, TILE // BLOCK, block, 0)
        here = pl.ds(tile * TILE, TILE)
        c0 = pltpu.make_async_copy(stage, fs_ref.at[g, :, here], stage_sem.at[0])
        c1 = pltpu.make_async_copy(stage.at[0], cb_ref.at[g, 0, here], stage_sem.at[1])
        c0.start()
        c1.start()
        c0.wait()
        c1.wait()

        for first, count in ((0, 1), (1, 1), (2, tiles - 2)):

            @pl.when(t == first + count - 1)
            def _():
                ready = pl.ds(first * TILE, count * TILE)
                for dl, dz in sends:
                    part = (0, dl * ord_count + dz, ready)
                    send(fs_ref, cb_ref, part, ahead(dl, dz), send_f.at[0], recv_f.at[0])

        @pl.when(t == 2 * tiles - 1)
        def _():
            send_forward(1)

        return carry

    lax.fori_loop(0, groups * tiles, forward_step, 0)

    def drain(ref, g, sem):
        far = ref.at[g, pl.ds(1, devices - 1)]
        pltpu.make_async_copy(far, far, sem).wait()

    lane = lax.broadcasted_iota(jnp.int32, (half, lanes), 1)
    low = lane < channels
    places = [(a, b) for a in range(lat_count) for b in range(ord_count)]

    def index_of(a, b):
        return (la + (lat_count - a)) % lat_count * ord_count + (oz + (ord_count - b)) % ord_count

    def slot_step(g, s):
        q = g * GROUP + s
        cur = q % 2

        @pl.when(q + 1 < slots)
        def _():
            leg_copy(q + 1, (q + 1) % 2).start()

        combos = [(p, t, a) for p in range(2) for t in range(ord_count // 2) for a in range(lat_count)]
        for p, t, a in combos:
            line = pl.ds(2 * s + p, half, stride=pair_rows)
            first = z[a * ord_count + 2 * t, line, :]
            second = z[a * ord_count + 2 * t + 1, line, :]
            at = slice(p * width + t * lanes, p * width + (t + 1) * lanes)
            rhs[a * 2 * half : a * 2 * half + half, at] = jnp.where(
                low, first, pltpu.roll(second, channels, 1)
            )
            rhs[a * 2 * half + half : (a + 1) * 2 * half, at] = jnp.where(
                low, pltpu.roll(first, channels, 1), second
            )

        leg_copy(q, cur).wait()
        order = rows_ref[pl.ds(2 * (first_slot + q), 1), :1]
        weight = 1.0 + jnp.minimum(order, 1.0)
        gain = gains[...]
        for k in reversed(range(order_bits)):
            shift = 1 << k
            bit = jnp.floor(order * (1.0 / shift)) - 2.0 * jnp.floor(order * (0.5 / shift))
            if shift >= 8:
                size = degrees + 8 + shift - 8
                gain = jnp.where(bit > 0.5, gain[shift : shift + size], gain[:size])
            else:
                gain = jnp.where(bit > 0.5, pltpu.roll(gain, gain.shape[0] - shift, 0), gain)
        gain = gain[:degrees]
        for p in range(2):
            at = slice(p * width, (p + 1) * width)
            spec = jnp.dot(legv[cur], rhs[:, at].astype(jnp.bfloat16), preferred_element_type=jnp.float32)
            filtered = (spec * gain).astype(jnp.bfloat16)
            mixed = jnp.dot(filtered, mixing_ref[...], preferred_element_type=jnp.float32)
            synth = lax.dot_general(
                legv[cur], mixed.astype(jnp.bfloat16), (((0,), (0,)), ((), ())),
                preferred_element_type=jnp.float32,
            )
            rhs[:, at] = synth * weight

        for p, t, a in combos:
            line = pl.ds(2 * s + p, half, stride=pair_rows)
            at = slice(p * width + t * lanes, p * width + (t + 1) * lanes)
            first = rhs[a * 2 * half : a * 2 * half + half, at]
            second = rhs[a * 2 * half + half : (a + 1) * 2 * half, at]
            z[a * ord_count + 2 * t, line, :] = jnp.where(low, first, pltpu.roll(second, channels, 1))
            z[a * ord_count + 2 * t + 1, line, :] = jnp.where(
                low, pltpu.roll(first, channels, 1), second
            )

    def middle_step(g, carry):
        drain(cb_ref, g, recv_f.at[g])

        @pl.when(g + 2 < groups)
        def _():
            send_forward(g + 2)

        @pl.when(g == groups - 2)
        def _():
            send_back(0)

        @pl.when(g == groups - 1)
        def _():
            for early in range(1, groups - 2):
                send_back(early)

        loads = [
            pltpu.make_async_copy(cb_ref.at[g, index_of(a, b)], av.at[j], a_sem.at[j])
            for j, (a, b) in enumerate(places)
        ]
        for c in loads:
            c.start()
        for c in loads:
            c.wait()

        def widen(j, carry):
            z[j] = av[j].reshape(half * pair_rows, lanes).astype(jnp.float32)
            return carry

        lax.fori_loop(0, devices, widen, 0)

        def per_slot(s, carry):
            slot_step(g, s)
            return carry

        lax.fori_loop(0, GROUP, per_slot, 0)

        def narrow(j, carry):
            av[j] = z[j].reshape(half, pair_rows, lanes).astype(jnp.bfloat16)
            return carry

        lax.fori_loop(0, devices, narrow, 0)
        stores = [
            pltpu.make_async_copy(av.at[j], ys_ref.at[g, index_of(a, b)], a_sem.at[j])
            for j, (a, b) in enumerate(places)
        ]
        own = pltpu.make_async_copy(av.at[la * ord_count + oz], yb_ref.at[g, 0], own_sem)
        for c in stores:
            c.start()
        own.start()
        for c in stores:
            c.wait()
        own.wait()

        @pl.when(g == groups - 1)
        def _():
            for k, (first, count) in enumerate(cuts):
                for late in (groups - 2, groups - 1):
                    for dl, dz in sends:
                        part = (late, dl * ord_count + dz, pl.ds(first * TILE, count * TILE))
                        send(ys_ref, yb_ref, part, behind(dl, dz), send_r.at[late], recv_last.at[k])

        return carry

    gain_copy.wait()
    lax.fori_loop(0, groups, middle_step, 0)

    for c in x_copies(0, 0):
        c.start()
    for g in range(groups - 2):
        drain(yb_ref, g, recv_r.at[g])

    def out_copies(c, slot):
        return [
            pltpu.make_async_copy(
                xv.at[slot, :, h], out_ref.at[pl.ds(h * half + c * TILE, TILE)], o_sem.at[slot, h]
            )
            for h in range(2)
        ]

    def inverse_step(c, carry):
        slot = c % 2
        for k, (first, count) in enumerate(cuts):

            @pl.when(c == first)
            def _():
                rows_here = pl.ds(first * TILE, count * TILE)
                far = yb_ref.at[pl.ds(groups - 2, 2), pl.ds(1, devices - 1), rows_here]
                pltpu.make_async_copy(far, far, recv_last.at[k]).wait()

        loads = [
            pltpu.make_async_copy(
                yb_ref.at[:, :, c * TILE + k], v.at[:, :, :, pl.ds(k * lanes, lanes)], v_sem.at[k]
            )
            for k in range(TILE)
        ]
        for copy in loads:
            copy.start()

        @pl.when(c >= 1)
        def _():
            for copy in out_copies(c - 1, 1 - slot):
                copy.wait()

        @pl.when(c + 1 < tiles)
        def _():
            for copy in x_copies(c + 1, 1 - slot):
                copy.start()

        for copy in x_copies(c, slot):
            copy.wait()
        for copy in loads:
            copy.wait()
        wide = BLOCK * lanes
        depth = groups * devices * pair_rows

        def block(kb, carry):
            cols = pl.ds(pl.multiple_of(kb * wide, wide), wide)
            back = lax.dot_general(
                v[:, :, :, cols].reshape(depth, wide),
                table_ref[...],
                (((0,), (0,)), ((), ())),
                preferred_element_type=jnp.float32,
            )
            here = pl.ds(kb * BLOCK, BLOCK)
            state = xv[slot, here].reshape(wide, lon_count).astype(jnp.float32)
            new = (state + jax.nn.gelu(back, approximate=True)).astype(jnp.bfloat16)
            xv[slot, here] = new.reshape(BLOCK, 2, channels, lon_count)
            return carry

        lax.fori_loop(0, TILE // BLOCK, block, 0)
        for copy in out_copies(c, slot):
            copy.start()
        return carry

    lax.fori_loop(0, tiles, inverse_step, 0)
    for copy in out_copies(tiles - 1, (tiles - 1) % 2):
        copy.wait()
    for g in range(groups):
        drain(fs_ref, g, send_f.at[g])
        drain(ys_ref, g, send_r.at[g])


def fast_shards(state_field, slot_order, legendre, degree_gain, mixing):
    channels, lat_rows, lon_count = state_field.shape
    slots, degrees, latitudes = legendre.shape
    width = mixing.shape[0]
    lat_count = lax.axis_size("lat")
    ord_count = lax.axis_size("ord")
    devices = lat_count * ord_count
    groups = slots // GROUP
    half = lat_rows // 2
    lanes = 2 * channels
    pair_rows = 2 * GROUP
    x = state_field.transpose(1, 0, 2)
    rows = jnp.broadcast_to(jnp.repeat(slot_order, 2)[:, None], (2 * devices * slots, 128)).astype(jnp.float32)
    order_bits = (devices * slots - 1).bit_length()
    sizes = (lat_count, ord_count, groups, half, channels, slots)
    buffer = jax.ShapeDtypeStruct((groups, devices, half, pair_rows, lanes), jnp.bfloat16)
    tiles = half // TILE
    anywhere = pl.BlockSpec(memory_space=pl.ANY)
    vmem = pl.BlockSpec(memory_space=pltpu.VMEM)
    sem = pltpu.SemaphoreType.DMA
    flops = 4 * devices * slots * channels * lat_rows * lon_count
    flops += 4 * slots * width * degrees * (2 * latitudes + width)
    outs = pl.pallas_call(
        functools.partial(whole_kernel, sizes),
        out_shape=[jax.ShapeDtypeStruct(x.shape, jnp.bfloat16)] + [buffer] * 4,
        in_specs=[anywhere, vmem, anywhere, anywhere, vmem],
        out_specs=[anywhere] * 5,
        scratch_shapes=[
            pltpu.VMEM((groups * devices * pair_rows, lon_count), jnp.bfloat16),
            pltpu.VMEM((degrees + (1 << order_bits), width), jnp.float32),
            pltpu.VMEM((2, TILE, 2, channels, lon_count), jnp.bfloat16),
            pltpu.VMEM((devices, TILE, pair_rows, lanes), jnp.bfloat16),
            pltpu.VMEM((devices, half, pair_rows, lanes), jnp.bfloat16),
            pltpu.VMEM((devices, half * pair_rows, lanes), jnp.float32),
            pltpu.VMEM((2, degrees, latitudes), jnp.bfloat16),
            pltpu.VMEM((latitudes, 2 * width), jnp.float32),
            pltpu.VMEM((groups, devices, pair_rows, TILE * lanes), jnp.bfloat16),
            sem,
            sem((2, 2)),
            sem((2,)),
            sem((devices,)),
            sem((2,)),
            sem((TILE,)),
            sem((2, 2)),
            sem,
            sem((groups,)),
            sem((groups,)),
            sem((groups,)),
            sem((groups,)),
            sem((len(cuts_of(tiles)),)),
        ],
        compiler_params=pltpu.CompilerParams(
            collective_id=0, has_side_effects=True, vmem_limit_bytes=58 * 1024 * 1024
        ),
        cost_estimate=pl.CostEstimate(flops=flops, bytes_accessed=10**9, transcendentals=0),
    )(x, rows, legendre, degree_gain, mixing)
    return outs[0].transpose(1, 0, 2)


def fits(mesh, state_field, legendre, mixing):
    lat_count, ord_count = mesh.shape["lat"], mesh.shape["ord"]
    channels = mixing.shape[0] // ord_count
    lat_rows = state_field.shape[1] // lat_count
    slots = legendre.shape[0] // (lat_count * ord_count)
    return (
        2 * channels == 128
        and ord_count % 2 == 0
        and lat_rows % (2 * TILE) == 0
        and lat_rows // (2 * TILE) > 2
        and slots % GROUP == 0
        and slots // GROUP > 2
        and state_field.shape[2] % 4 == 0
    )


def solution(mesh):
    placed = (P(("batch", "ord"), "lat", None), P(), P(("lat", "ord"), None, None), P(), P())

    def run(state_field, slot_order, legendre, degree_gain, mixing):
        shards = fast_shards if fits(mesh, state_field, legendre, mixing) else plain_shards
        return jax.shard_map(
            shards,
            mesh=mesh,
            in_specs=placed,
            out_specs=P(("batch", "ord"), "lat", None),
            check_vma=False,
        )(state_field, slot_order, legendre, degree_gain, mixing)

    return run
```

```python
import functools
import math

import jax
import jax.numpy as jnp
from jax import lax
from jax.experimental import pallas as pl
from jax.experimental.pallas import tpu as pltpu
from jax.sharding import PartitionSpec as P

CHUNKS = 4


def table(orders, lon_count):
    longitude = lax.broadcasted_iota(jnp.int32, orders.shape + (lon_count,), orders.ndim)
    product = (orders[..., None] * longitude).astype(jnp.float32)
    turns = jnp.floor((product + 0.5) * (1.0 / lon_count))
    angle = (product - turns * lon_count) * (2.0 * math.pi / lon_count)
    root = 1.0 / math.sqrt(lon_count)
    return (jnp.cos(angle) * root).astype(jnp.bfloat16), (-jnp.sin(angle) * root).astype(jnp.bfloat16)


def middle_kernel(orders_ref, coeffs_ref, legendre_ref, gain_ref, mixing_ref, out_ref):
    order = orders_ref[pl.program_id(0)]
    slot_table = legendre_ref[0]
    mixing = mixing_ref[...]
    degrees = slot_table.shape[0]
    width = mixing.shape[0]
    weight = jnp.where(order == 0, 1.0, 2.0).astype(jnp.float32)
    kept = lax.broadcasted_iota(jnp.int32, (degrees, width), 0) < degrees - order
    start = pl.multiple_of(order // 8 * 8, 8)
    window = gain_ref[pl.ds(start, degrees + 8), :]
    gain = pltpu.roll(window, degrees + 8 - order % 8, 0)[:degrees]
    for part in range(2):
        spec = lax.dot_general(
            slot_table, coeffs_ref[0, part], (((1,), (0,)), ((), ())), preferred_element_type=jnp.float32
        )
        filtered = jnp.where(kept, spec * gain, 0.0).astype(jnp.bfloat16)
        mixed = jnp.dot(filtered, mixing, preferred_element_type=jnp.float32).astype(jnp.bfloat16)
        synth = lax.dot_general(
            slot_table, mixed, (((0,), (0,)), ((), ())), preferred_element_type=jnp.float32
        )
        out_ref[0, part] = (synth * weight).astype(jnp.bfloat16)


def middle(orders, coeffs, legendre, first, padded_gain, mixing):
    slots, parts, latitudes, width = coeffs.shape
    degrees = legendre.shape[1]
    return pl.pallas_call(
        middle_kernel,
        out_shape=jax.ShapeDtypeStruct(coeffs.shape, jnp.bfloat16),
        grid_spec=pltpu.PrefetchScalarGridSpec(
            num_scalar_prefetch=1,
            grid=(slots,),
            in_specs=[
                pl.BlockSpec((1, parts, latitudes, width), lambda s, o: (s, 0, 0, 0)),
                pl.BlockSpec((1, degrees, latitudes), lambda s, o: (first + s, 0, 0)),
                pl.BlockSpec(padded_gain.shape, lambda s, o: (0, 0)),
                pl.BlockSpec(mixing.shape, lambda s, o: (0, 0)),
            ],
            out_specs=pl.BlockSpec((1, parts, latitudes, width), lambda s, o: (s, 0, 0, 0)),
        ),
        compiler_params=pltpu.CompilerParams(vmem_limit_bytes=40 * 1024 * 1024),
        cost_estimate=pl.CostEstimate(
            flops=2 * slots * parts * width * degrees * (2 * latitudes + width),
            bytes_accessed=2 * slots * latitudes * (2 * parts * width + degrees),
            transcendentals=0,
        ),
    )(orders, coeffs, legendre, padded_gain, mixing)


def plain_shards(state_field, slot_order, legendre, degree_gain, mixing):
    channels, lat_rows, lon_count = state_field.shape
    all_slots = slot_order.shape[0]
    my_slots, degrees, latitudes = legendre.shape
    width = mixing.shape[0]
    lat_count = lax.axis_size("lat")
    ord_count = lax.axis_size("ord")
    devices = lat_count * ord_count
    chunks = math.gcd(CHUNKS, my_slots)
    piece = my_slots // chunks
    rows = channels * lat_rows
    me = lax.axis_index(("lat", "ord"))
    grid_rows = state_field.transpose(1, 0, 2).reshape(rows, lon_count)
    orders_by_device = slot_order.reshape(devices, chunks, piece)
    padded_gain = jnp.concatenate([degree_gain, jnp.zeros((degrees + 8, width), jnp.float32)], axis=0)

    tables = []
    arrived = []
    for g in range(chunks):
        cosine, sine = table(orders_by_device[:, g], lon_count)
        rows_here = jnp.stack([cosine, sine], axis=1).reshape(2 * devices * piece, lon_count)
        tables.append(rows_here)
        fourier = lax.dot_general(
            rows_here, grid_rows, (((1,), (1,)), ((), ())), preferred_element_type=jnp.float32
        ).astype(jnp.bfloat16)
        arrived.append(
            lax.all_to_all(
                fourier.reshape(devices, 2 * piece, rows),
                ("lat", "ord"),
                split_axis=0,
                concat_axis=0,
                tiled=True,
            )
        )

    returned = []
    for g in range(chunks):
        coeffs = arrived[g].reshape(lat_count, ord_count, 2, piece, lat_rows, channels)
        coeffs = coeffs.transpose(3, 2, 0, 4, 1, 5).reshape(piece, 2, latitudes, width)
        orders_here = lax.dynamic_slice_in_dim(slot_order, me * my_slots + g * piece, piece, 0)
        synth = middle(orders_here, coeffs, legendre, g * piece, padded_gain, mixing)
        outgoing = synth.reshape(piece, 2, lat_count, lat_rows, ord_count, channels)
        outgoing = outgoing.transpose(2, 4, 1, 0, 3, 5).reshape(devices, 2 * piece, rows)
        returned.append(
            lax.all_to_all(outgoing, ("lat", "ord"), split_axis=0, concat_axis=0, tiled=True).reshape(
                2 * devices * piece, rows
            )
        )

    back = lax.dot_general(
        jnp.concatenate(returned, axis=0),
        jnp.concatenate(tables, axis=0),
        (((0,), (0,)), ((), ())),
        preferred_element_type=jnp.float32,
    )
    back = back.reshape(lat_rows, channels, lon_count).transpose(1, 0, 2)
    return (state_field.astype(jnp.float32) + jax.nn.gelu(back, approximate=True)).astype(
        jnp.bfloat16
    )


MESH = pl.DeviceIdType.MESH
GROUP = 8
TILE = 10
BLOCK = 5


def order_of_sends(lat_count, ord_count):
    steps = sorted(range(ord_count), key=lambda dz: (dz == 0, abs(2 * dz - ord_count)))
    return [(dl, dz) for dz in steps for dl in range(lat_count) if (dl, dz) != (0, 0)]


def cuts_of(tiles):
    counts = []
    while sum(counts) < tiles:
        counts.insert(0, min(len(counts) // 2 + 1, tiles - sum(counts)))
    return [(sum(counts[:k]), count) for k, count in enumerate(counts)]


def cosine(phase, lon_count):
    turns = jnp.floor((phase + 0.5) * (1.0 / lon_count))
    fold = jnp.abs(phase - turns * lon_count - lon_count // 2) - lon_count // 4
    angle = fold * (2.0 * math.pi / lon_count)
    square = angle * angle
    series = 1.0 / math.factorial(13)
    for n in (11, 9, 7, 5, 3, 1):
        series = series * square + (-1.0) ** (n // 2) / math.factorial(n)
    return series * angle


def whole_kernel(
    sizes, x_ref, rows_ref, legendre_ref, degree_gain_ref, mixing_ref,
    out_ref, fs_ref, cb_ref, ys_ref, yb_ref,
    table_ref, gains, xv, stage, av, z, legv, rhs, v,
    gain_sem, x_sem, stage_sem, a_sem, leg_sem, v_sem, o_sem, own_sem,
    send_f, recv_f, send_r, recv_r, recv_last,
):
    lat_count, ord_count, groups, half, channels, slots = sizes
    devices = lat_count * ord_count
    lanes = 2 * channels
    pair_rows = 2 * GROUP
    width = ord_count * channels
    degrees = legendre_ref.shape[1]
    order_bits = (devices * slots - 1).bit_length()
    lon_count = x_ref.shape[2]
    tiles = half // TILE
    la = lax.axis_index("lat")
    oz = lax.axis_index("ord")
    bt = lax.axis_index("batch")
    first_slot = (la * ord_count + oz) * slots
    sends = order_of_sends(lat_count, ord_count)
    cuts = cuts_of(tiles)

    def ahead(dl, dz):
        return ((la + dl) % lat_count, (oz + dz) % ord_count, bt)

    def behind(dl, dz):
        return ((la + (lat_count - dl)) % lat_count, (oz + (ord_count - dz)) % ord_count, bt)

    def x_copies(tile, slot):
        return [
            pltpu.make_async_copy(
                x_ref.at[pl.ds(h * half + tile * TILE, TILE)], xv.at[slot, :, h], x_sem.at[slot, h]
            )
            for h in range(2)
        ]

    def leg_copy(q, slot):
        return pltpu.make_async_copy(legendre_ref.at[q], legv.at[slot], leg_sem.at[slot])

    for c in x_copies(0, 0):
        c.start()
    leg_copy(0, 0).start()
    gain_copy = pltpu.make_async_copy(degree_gain_ref, gains.at[pl.ds(0, degrees)], gain_sem)
    gain_copy.start()
    gains[degrees:, :] = jnp.zeros((gains.shape[0] - degrees, width), jnp.float32)

    barrier = pltpu.get_barrier_semaphore()
    for dl, dz in sends:
        pl.semaphore_signal(barrier, inc=1, device_id=ahead(dl, dz), device_id_type=MESH)
    pl.semaphore_wait(barrier, devices - 1)

    def send(src, dst, part, dest, ssem, rsem):
        pltpu.make_async_remote_copy(
            src_ref=src.at[part], dst_ref=dst.at[part], send_sem=ssem, recv_sem=rsem,
            device_id=dest, device_id_type=MESH,
        ).start()

    def send_forward(g):
        for dl, dz in sends:
            part = (g, dl * ord_count + dz)
            send(fs_ref, cb_ref, part, ahead(dl, dz), send_f.at[g], recv_f.at[g])

    def send_back(g):
        for dl, dz in sends:
            part = (g, dl * ord_count + dz)
            send(ys_ref, yb_ref, part, behind(dl, dz), send_r.at[g], recv_r.at[g])

    def table_block(g, k):
        here = pl.ds(pl.multiple_of((g * devices + k) * pair_rows, pair_rows), pair_rows)
        dl, dz = k // ord_count, k % ord_count
        owner = (la + dl) % lat_count * ord_count + (oz + dz) % ord_count
        theirs = (owner * slots + g * GROUP) * 2
        order = rows_ref[pl.ds(pl.multiple_of(theirs, pair_rows), pair_rows), :1]
        shape = (pair_rows, lon_count)
        part = (lax.broadcasted_iota(jnp.int32, shape, 0) % 2).astype(jnp.float32)
        longitude = lax.broadcasted_iota(jnp.int32, shape, 1).astype(jnp.float32)
        values = cosine(order * longitude + part * (lon_count // 4), lon_count)
        table_ref[here, :] = (values * (1.0 / math.sqrt(lon_count))).astype(jnp.bfloat16)

    def forward_step(t, carry):
        g = t // tiles

        @pl.when(t % tiles == 0)
        def _():
            def per_device(k, carry):
                table_block(g, k)
                return carry

            lax.fori_loop(0, devices, per_device, 0)

        table_rows = pl.ds(pl.multiple_of(g * devices * pair_rows, devices * pair_rows), devices * pair_rows)
        tile = t % tiles
        slot = t % 2

        @pl.when(t + 1 < groups * tiles)
        def _():
            for c in x_copies((t + 1) % tiles, (t + 1) % 2):
                c.start()

        for c in x_copies(tile, slot):
            c.wait()

        def block(kb, carry):
            rows = xv[slot, pl.ds(kb * BLOCK, BLOCK)].reshape(BLOCK * lanes, lon_count)
            res = lax.dot_general(
                table_ref[table_rows, :], rows, (((1,), (1,)), ((), ())), preferred_element_type=jnp.float32
            )
            for k in range(BLOCK):
                piece = res[:, k * lanes : (k + 1) * lanes].reshape(devices, pair_rows, lanes)
                stage[:, kb * BLOCK + k] = piece.astype(jnp.bfloat16)
            return carry

        lax.fori_loop(0, TILE // BLOCK, block, 0)
        here = pl.ds(tile * TILE, TILE)
        c0 = pltpu.make_async_copy(stage, fs_ref.at[g, :, here], stage_sem.at[0])
        c1 = pltpu.make_async_copy(stage.at[0], cb_ref.at[g, 0, here], stage_sem.at[1])
        c0.start()
        c1.start()
        c0.wait()
        c1.wait()

        for first, count in ((0, 1), (1, 2), (3, 3), (6, tiles - 6)):

            @pl.when(t == first + count - 1)
            def _():
                ready = pl.ds(first * TILE, count * TILE)
                for dl, dz in sends:
                    part = (0, dl * ord_count + dz, ready)
                    send(fs_ref, cb_ref, part, ahead(dl, dz), send_f.at[0], recv_f.at[0])

        @pl.when(t == 2 * tiles - 1)
        def _():
            send_forward(1)

        return carry

    lax.fori_loop(0, groups * tiles, forward_step, 0)

    def drain(ref, g, sem):
        far = ref.at[g, pl.ds(1, devices - 1)]
        pltpu.make_async_copy(far, far, sem).wait()

    lane = lax.broadcasted_iota(jnp.int32, (half, lanes), 1)
    low = lane < channels
    places = [(a, b) for a in range(lat_count) for b in range(ord_count)]

    def index_of(a, b):
        return (la + (lat_count - a)) % lat_count * ord_count + (oz + (ord_count - b)) % ord_count

    def slot_step(g, s):
        q = g * GROUP + s
        cur = q % 2

        @pl.when(q + 1 < slots)
        def _():
            leg_copy(q + 1, (q + 1) % 2).start()

        combos = [(p, t, a) for p in range(2) for t in range(ord_count // 2) for a in range(lat_count)]
        for p, t, a in combos:
            line = pl.ds(2 * s + p, half, stride=pair_rows)
            first = z[a * ord_count + 2 * t, line, :]
            second = z[a * ord_count + 2 * t + 1, line, :]
            at = slice(p * width + t * lanes, p * width + (t + 1) * lanes)
            rhs[a * 2 * half : a * 2 * half + half, at] = jnp.where(
                low, first, pltpu.roll(second, channels, 1)
            )
            rhs[a * 2 * half + half : (a + 1) * 2 * half, at] = jnp.where(
                low, pltpu.roll(first, channels, 1), second
            )

        leg_copy(q, cur).wait()
        order = rows_ref[pl.ds(2 * (first_slot + q), 1), :1]
        weight = 1.0 + jnp.minimum(order, 1.0)
        gain = gains[...]
        for k in reversed(range(order_bits)):
            shift = 1 << k
            bit = jnp.floor(order * (1.0 / shift)) - 2.0 * jnp.floor(order * (0.5 / shift))
            if shift >= 8:
                size = degrees + 8 + shift - 8
                gain = jnp.where(bit > 0.5, gain[shift : shift + size], gain[:size])
            else:
                gain = jnp.where(bit > 0.5, pltpu.roll(gain, gain.shape[0] - shift, 0), gain)
        gain = gain[:degrees]
        for p in range(2):
            at = slice(p * width, (p + 1) * width)
            spec = jnp.dot(legv[cur], rhs[:, at].astype(jnp.bfloat16), preferred_element_type=jnp.float32)
            filtered = (spec * gain).astype(jnp.bfloat16)
            mixed = jnp.dot(filtered, mixing_ref[...], preferred_element_type=jnp.float32)
            synth = lax.dot_general(
                legv[cur], mixed.astype(jnp.bfloat16), (((0,), (0,)), ((), ())),
                preferred_element_type=jnp.float32,
            )
            rhs[:, at] = synth * weight

        for p, t, a in combos:
            line = pl.ds(2 * s + p, half, stride=pair_rows)
            at = slice(p * width + t * lanes, p * width + (t + 1) * lanes)
            first = rhs[a * 2 * half : a * 2 * half + half, at]
            second = rhs[a * 2 * half + half : (a + 1) * 2 * half, at]
            z[a * ord_count + 2 * t, line, :] = jnp.where(low, first, pltpu.roll(second, channels, 1))
            z[a * ord_count + 2 * t + 1, line, :] = jnp.where(
                low, pltpu.roll(first, channels, 1), second
            )

    def middle_step(g, carry):
        drain(cb_ref, g, recv_f.at[g])

        @pl.when(g + 2 < groups)
        def _():
            send_forward(g + 2)

        @pl.when(g == groups - 2)
        def _():
            send_back(0)

        @pl.when(g == groups - 1)
        def _():
            for early in range(1, groups - 2):
                send_back(early)

        loads = [
            pltpu.make_async_copy(cb_ref.at[g, index_of(a, b)], av.at[j], a_sem.at[j])
            for j, (a, b) in enumerate(places)
        ]
        for c in loads:
            c.start()
        for c in loads:
            c.wait()

        def widen(j, carry):
            z[j] = av[j].reshape(half * pair_rows, lanes).astype(jnp.float32)
            return carry

        lax.fori_loop(0, devices, widen, 0)

        def per_slot(s, carry):
            slot_step(g, s)
            return carry

        lax.fori_loop(0, GROUP, per_slot, 0)

        def narrow(j, carry):
            av[j] = z[j].reshape(half, pair_rows, lanes).astype(jnp.bfloat16)
            return carry

        lax.fori_loop(0, devices, narrow, 0)
        stores = [
            pltpu.make_async_copy(av.at[j], ys_ref.at[g, index_of(a, b)], a_sem.at[j])
            for j, (a, b) in enumerate(places)
        ]
        own = pltpu.make_async_copy(av.at[la * ord_count + oz], yb_ref.at[g, 0], own_sem)
        for c in stores:
            c.start()
        own.start()
        for c in stores:
            c.wait()
        own.wait()

        @pl.when(g == groups - 1)
        def _():
            for k, (first, count) in enumerate(cuts):
                for late in (groups - 2, groups - 1):
                    for dl, dz in sends:
                        part = (late, dl * ord_count + dz, pl.ds(first * TILE, count * TILE))
                        send(ys_ref, yb_ref, part, behind(dl, dz), send_r.at[late], recv_last.at[k])

        return carry

    gain_copy.wait()
    lax.fori_loop(0, groups, middle_step, 0)

    for c in x_copies(0, 0):
        c.start()
    for g in range(groups - 2):
        drain(yb_ref, g, recv_r.at[g])

    def out_copies(c, slot):
        return [
            pltpu.make_async_copy(
                xv.at[slot, :, h], out_ref.at[pl.ds(h * half + c * TILE, TILE)], o_sem.at[slot, h]
            )
            for h in range(2)
        ]

    def inverse_step(c, carry):
        slot = c % 2
        for k, (first, count) in enumerate(cuts):

            @pl.when(c == first)
            def _():
                rows_here = pl.ds(first * TILE, count * TILE)
                far = yb_ref.at[pl.ds(groups - 2, 2), pl.ds(1, devices - 1), rows_here]
                pltpu.make_async_copy(far, far, recv_last.at[k]).wait()

        loads = [
            pltpu.make_async_copy(
                yb_ref.at[:, :, c * TILE + k], v.at[:, :, :, pl.ds(k * lanes, lanes)], v_sem.at[k]
            )
            for k in range(TILE)
        ]
        for copy in loads:
            copy.start()

        @pl.when(c >= 1)
        def _():
            for copy in out_copies(c - 1, 1 - slot):
                copy.wait()

        @pl.when(c + 1 < tiles)
        def _():
            for copy in x_copies(c + 1, 1 - slot):
                copy.start()

        for copy in x_copies(c, slot):
            copy.wait()
        for copy in loads:
            copy.wait()
        wide = BLOCK * lanes
        depth = groups * devices * pair_rows

        def block(kb, carry):
            cols = pl.ds(pl.multiple_of(kb * wide, wide), wide)
            back = lax.dot_general(
                v[:, :, :, cols].reshape(depth, wide),
                table_ref[...],
                (((0,), (0,)), ((), ())),
                preferred_element_type=jnp.float32,
            )
            here = pl.ds(kb * BLOCK, BLOCK)
            state = xv[slot, here].reshape(wide, lon_count).astype(jnp.float32)
            new = (state + jax.nn.gelu(back, approximate=True)).astype(jnp.bfloat16)
            xv[slot, here] = new.reshape(BLOCK, 2, channels, lon_count)
            return carry

        lax.fori_loop(0, TILE // BLOCK, block, 0)
        for copy in out_copies(c, slot):
            copy.start()
        return carry

    lax.fori_loop(0, tiles, inverse_step, 0)
    for copy in out_copies(tiles - 1, (tiles - 1) % 2):
        copy.wait()
    for g in range(groups):
        drain(fs_ref, g, send_f.at[g])
        drain(ys_ref, g, send_r.at[g])


def fast_shards(state_field, slot_order, legendre, degree_gain, mixing):
    channels, lat_rows, lon_count = state_field.shape
    slots, degrees, latitudes = legendre.shape
    width = mixing.shape[0]
    lat_count = lax.axis_size("lat")
    ord_count = lax.axis_size("ord")
    devices = lat_count * ord_count
    groups = slots // GROUP
    half = lat_rows // 2
    lanes = 2 * channels
    pair_rows = 2 * GROUP
    x = state_field.transpose(1, 0, 2)
    rows = jnp.broadcast_to(jnp.repeat(slot_order, 2)[:, None], (2 * devices * slots, 128)).astype(jnp.float32)
    order_bits = (devices * slots - 1).bit_length()
    sizes = (lat_count, ord_count, groups, half, channels, slots)
    buffer = jax.ShapeDtypeStruct((groups, devices, half, pair_rows, lanes), jnp.bfloat16)
    tiles = half // TILE
    anywhere = pl.BlockSpec(memory_space=pl.ANY)
    vmem = pl.BlockSpec(memory_space=pltpu.VMEM)
    sem = pltpu.SemaphoreType.DMA
    flops = 4 * devices * slots * channels * lat_rows * lon_count
    flops += 4 * slots * width * degrees * (2 * latitudes + width)
    outs = pl.pallas_call(
        functools.partial(whole_kernel, sizes),
        out_shape=[jax.ShapeDtypeStruct(x.shape, jnp.bfloat16)] + [buffer] * 4,
        in_specs=[anywhere, vmem, anywhere, anywhere, vmem],
        out_specs=[anywhere] * 5,
        scratch_shapes=[
            pltpu.VMEM((groups * devices * pair_rows, lon_count), jnp.bfloat16),
            pltpu.VMEM((degrees + (1 << order_bits), width), jnp.float32),
            pltpu.VMEM((2, TILE, 2, channels, lon_count), jnp.bfloat16),
            pltpu.VMEM((devices, TILE, pair_rows, lanes), jnp.bfloat16),
            pltpu.VMEM((devices, half, pair_rows, lanes), jnp.bfloat16),
            pltpu.VMEM((devices, half * pair_rows, lanes), jnp.float32),
            pltpu.VMEM((2, degrees, latitudes), jnp.bfloat16),
            pltpu.VMEM((latitudes, 2 * width), jnp.float32),
            pltpu.VMEM((groups, devices, pair_rows, TILE * lanes), jnp.bfloat16),
            sem,
            sem((2, 2)),
            sem((2,)),
            sem((devices,)),
            sem((2,)),
            sem((TILE,)),
            sem((2, 2)),
            sem,
            sem((groups,)),
            sem((groups,)),
            sem((groups,)),
            sem((groups,)),
            sem((len(cuts_of(tiles)),)),
        ],
        compiler_params=pltpu.CompilerParams(
            collective_id=0, has_side_effects=True, vmem_limit_bytes=58 * 1024 * 1024
        ),
        cost_estimate=pl.CostEstimate(flops=flops, bytes_accessed=10**9, transcendentals=0),
    )(x, rows, legendre, degree_gain, mixing)
    return outs[0].transpose(1, 0, 2)


def fits(mesh, state_field, legendre, mixing):
    lat_count, ord_count = mesh.shape["lat"], mesh.shape["ord"]
    channels = mixing.shape[0] // ord_count
    lat_rows = state_field.shape[1] // lat_count
    slots = legendre.shape[0] // (lat_count * ord_count)
    return (
        2 * channels == 128
        and ord_count % 2 == 0
        and lat_rows % (2 * TILE) == 0
        and lat_rows // (2 * TILE) > 6
        and slots % GROUP == 0
        and slots // GROUP > 2
        and state_field.shape[2] % 4 == 0
    )


def solution(mesh):
    placed = (P(("batch", "ord"), "lat", None), P(), P(("lat", "ord"), None, None), P(), P())

    def run(state_field, slot_order, legendre, degree_gain, mixing):
        shards = fast_shards if fits(mesh, state_field, legendre, mixing) else plain_shards
        return jax.shard_map(
            shards,
            mesh=mesh,
            in_specs=placed,
            out_specs=P(("batch", "ord"), "lat", None),
            check_vma=False,
        )(state_field, slot_order, legendre, degree_gain, mixing)

    return run
```
